32 devices in a mesh: parts: 2 (over y), wide: 4 (over z), mp: 4 (over x, core).
Axes of the slice: x: 2, y: 2, z: 4, core: 2. Of those that a mesh axis runs over, the one named last changes fastest.
Arguments:
- prompt_states: bfloat16 [4096, 8192], P(('parts', 'wide'), 'mp'), parts along dimension 0, may hold values from -6 to 6
- norm_gain: float32 [8192], P('mp'), may hold values from 0.1 to 1.9
- kv_weight: bfloat16 [8192, 2048], P('mp', 'wide'), may hold values from -0.0625 to 0.0625
- block_owner: int32 [256, 1], P(('parts', 'wide')), parts along dimension 0, may hold values from 0 to 3; in each aligned block of 32 rows (0 to 31, 32 to 63, ...) at most 16 rows name the same one
- block_request: int32 [256], P(('parts', 'wide')), parts along dimension 0, may hold values from 0 to 1
- block_admit: int32 [256], P(('parts', 'wide')), parts along dimension 0, may hold values 0 or 1
- cache_kv: bfloat16 [16, 2048, 2048], P(('parts', 'wide'), None, 'mp'), parts along dimension 0, may hold values from -6 to 6
- cache_len: int32 [16], P(('parts', 'wide')), parts along dimension 0, may hold values from 1 to 2048
- queries: bfloat16 [16, 4, 8192], P(('parts', 'wide'), None, 'mp'), parts along dimension 0, may hold values from -128 to 128
- draft_kv: bfloat16 [16, 4, 2048], P(('parts', 'wide'), None, 'mp'), parts along dimension 0, may hold values from -8 to 8
Outputs:
- attended: bfloat16 [16, 4, 8192], P(('parts', 'wide'), None, 'mp'), parts along dimension 0
The draws below stay inside these ranges and needn't reach their ends.
There are 2 independent parts, one for each index of `parts`. The reference program is written for one: setup_inputs(seed, part) draws one part's arguments, and reference() takes and returns one part's arrays. A program takes and returns all parts, laid end to end along the dimension named above; an argument that names none is the same for every part. Nothing has to cross between parts.
Inputs may be any that keep to these rules, and one draw needn't show every extreme that they name: `block_owner`: in each prefill group's 32 blocks no owner is named more than 16 times, a bound that some block reaches.
All inputs are finite; a program needn't handle non-finite values. No bound on the sum of `block_admit` on one device may be relied on, other than what follows from the above.
Results may differ from the reference program's by a relative error of at most 0.019.
Values may be sent and summed in bfloat16 or wider, within the bound.
No kernel may reach another device: no remote copies, remote signals or barrier semaphores. Data moves between devices by JAX's collectives and lax.ppermute only.
A program may use at most 64 MiB of HBM per device.

```python
import math
import jax
import jax.numpy as jnp
import numpy as np
from jax import lax

D = 8192
KVH = 8
HD = 128
QH = 64
KVW = 2048
BLK = 16
PBLK = 32
CAP = 16
REQ_DEV = 2
CACHE = 2048
STEPS = 4
PTOKENS = 2048
PBLOCKS = 128
REQUESTS = 8
N_WIDE = 4
N_MP = 4


def joint_draw(key):
    base = jax.random.fold_in(key, 7101)
    key_draft, key_query = jax.random.split(base, 2)
    groups = QH // KVH
    draft = jnp.clip(jax.random.normal(key_draft, (REQUESTS, STEPS, KVH, 2, HD), jnp.float32), -6.0, 6.0)
    query = jnp.clip(jax.random.normal(key_query, (REQUESTS, STEPS, KVH, groups, HD), jnp.float32), -6.0, 6.0)
    return (query.reshape(REQUESTS, STEPS, QH * HD), draft.reshape(REQUESTS, STEPS, KVH * 2 * HD))


def draw_queries(key, part):
    return joint_draw(key)[0].astype(jnp.bfloat16)


def draw_draft_kv(key, part):
    return joint_draw(key)[1].astype(jnp.bfloat16)


def with_ends(array, own_key, low, high):
    index_at = [jax.random.randint(jax.random.fold_in(own_key, axis), (), 0, length) for axis, length in enumerate(array.shape)]
    widest = array.shape.index(max(array.shape))
    beside = index_at[:widest] + [(index_at[widest] + 1) % array.shape[widest]] + index_at[widest + 1:]
    return array.at[tuple(index_at)].set(low).at[tuple(beside)].set(high)


def block_scale(key, dims, cuts, smallest, largest):
    factor_of, own = 1.0, jax.random.fold_in(key, 6)
    for dim, shards_of in cuts:
        draws = jnp.exp(jax.random.uniform(jax.random.fold_in(own, dim), (shards_of,), jnp.float32, smallest / len(cuts), largest / len(cuts)))
        factor_of = factor_of * jnp.repeat(draws, dims[dim] // shards_of).reshape([-1 if axis == dim else 1 for axis in range(len(dims))])
    return factor_of


def shared_out(key, own, number, rows, count, top, most, slope):
    ranking = jax.random.permutation(key, count)
    heavy_load, ordinary = shares(count, rows * top, most, slope, True), shares(count, rows * top, most, slope, False)
    places = jnp.arange(count)

    def named(sizes, rotation):
        used = int((sizes > 0).sum())
        fixed = max(1, used // 4)
        moved = fixed + (places - fixed + rotation * (used - fixed)) % max(1, count - fixed)
        return jnp.zeros((count,), jnp.int32).at[ranking[jnp.where(places < fixed, places, moved)]].set(jnp.asarray(sizes, jnp.int32))

    sizes = jnp.where(number % 4 == 0, named(heavy_load, number // 4), named(ordinary, number - number // 4 - 1))
    mixed = jax.random.permutation(jax.random.fold_in(own, 3), count)
    giver, receiver = mixed[0:count // 2 * 2:2], mixed[1:count // 2 * 2:2]
    room = jnp.minimum(sizes[giver] - 1, most - sizes[receiver]) // 2
    room = jnp.where((giver == ranking[0]) | (receiver == ranking[0]) | (sizes[receiver] == 0), 0, jnp.maximum(room, 0))
    moved = jax.random.randint(jax.random.fold_in(own, 4), (count // 2,), 0, 1 << 20) % (room + 1)
    sizes = sizes.at[giver].add(-moved).at[receiver].add(moved)
    items = jnp.searchsorted(jnp.cumsum(sizes), jnp.arange(rows * top), side="right").astype(jnp.int32)
    listing = items.reshape(top, rows).T
    listing = listing[jax.random.permutation(jax.random.fold_in(own, 1), rows)]
    rotation = jax.random.randint(jax.random.fold_in(own, 2), (rows, 1), 0, top)
    return jnp.take_along_axis(listing, (jnp.arange(top)[None, :] + rotation) % top, axis=1)


def shares(count, total, reach, skew, full):
    portions = [(1 << 20) // math.isqrt(grade ** skew) + 1 for grade in range(1, count + 1)]
    largest = reach if full else min(reach, max(-(-total // count), total * portions[0] // sum(portions)))
    least = 1 if total - largest >= count - 1 else 0
    counts, rest = [largest] + [least] * (count - 1), total - largest - least * (count - 1)
    while rest > 0:
        candidates = [i for i in range(1, count) if counts[i] < largest] or [i for i in range(1, count) if counts[i] < reach]
        pool, budget = sum([portions[i] for i in candidates]), rest
        for i in candidates:
            more = min(reach - counts[i], max(1, budget * portions[i] // pool), rest)
            counts[i] = counts[i] + more
            rest = rest - more
    return np.array(counts)


def noise(rng, shape, deviation, limit, pieces=(), kind=jnp.bfloat16):
    values = jax.random.normal(rng, shape, jnp.float32) * deviation
    if len(pieces) > 0:
        values = block_scale(rng, shape, pieces, -0.22, 0.18) * values
    return jnp.clip(values, min=-limit, max=limit).astype(kind)


def setup_inputs(seed: int = 0, part: int = 0) -> dict:
    arg_keys = jax.random.split(jax.random.key(seed), 11)
    part_splits = jax.random.split(jax.random.fold_in(arg_keys[10], part), 11)
    prompt_states = noise(part_splits[0], (PTOKENS, D), 1.0, 6.0, ((0, 4), (1, 4)))
    norm_gain = jnp.clip(1.0 + 0.18 * jax.random.normal(arg_keys[1], (D,), jnp.float32), 0.1, 1.9)
    kv_weight = noise(arg_keys[2], (D, KVW), D ** -0.5, 0.0625, ((0, 4), (1, 4)))
    block_owner_keys = jax.random.split(jax.random.fold_in(part_splits[3], 1), PBLOCKS // PBLK)
    block_owner_turns = jax.random.permutation(jax.random.fold_in(part_splits[3], 3), PBLOCKS // PBLK)
    block_owner = jax.vmap(lambda own, number: shared_out(jax.random.fold_in(part_splits[3], 2), own, number, PBLK, N_WIDE, 1, CAP, 2))(block_owner_keys, block_owner_turns).reshape((PBLOCKS, 1))
    block_request = with_ends(jax.random.randint(part_splits[4], (PBLOCKS,), 0, REQ_DEV), jax.random.fold_in(part_splits[4], 1), 0, REQ_DEV - 1).astype(jnp.int32)
    block_admit = with_ends((jax.random.randint(part_splits[5], (PBLOCKS,), 0, 4) < 3).astype(jnp.int32), jax.random.fold_in(part_splits[5], 1), 0, 1)
    cache_kv = noise(part_splits[6], (REQUESTS, CACHE, KVW), 1.0, 6.0, ((0, 4), (2, 4)))
    cache_len = with_ends(jax.random.randint(part_splits[7], (REQUESTS,), 1, CACHE + 1), jax.random.fold_in(part_splits[7], 1), 1, CACHE).astype(jnp.int32)
    queries = draw_queries(jax.random.fold_in(jax.random.fold_in(arg_keys[10], part), 71), part)
    draft_kv = draw_draft_kv(jax.random.fold_in(jax.random.fold_in(arg_keys[10], part), 71), part)
    return dict(prompt_states=prompt_states, norm_gain=norm_gain, kv_weight=kv_weight, block_owner=block_owner, block_request=block_request, block_admit=block_admit, cache_kv=cache_kv, cache_len=cache_len, queries=queries, draft_kv=draft_kv)


def reference(prompt_states, norm_gain, kv_weight, block_owner, block_request, block_admit, cache_kv, cache_len, queries, draft_kv):
    states = prompt_states.astype(jnp.float32)
    inverse = lax.rsqrt(lax.optimization_barrier(jnp.mean(states * states, axis=1)) + 1e-05)
    scaled = (states * norm_gain).astype(jnp.bfloat16)
    slice_width = D // N_MP
    projected = jnp.zeros((PTOKENS, KVW), jnp.float32)
    for index in range(N_MP):
        lower = index * slice_width
        partial_value = jnp.dot(scaled[:, lower:lower + slice_width], kv_weight[lower:lower + slice_width], preferred_element_type=jnp.float32)
        projected = projected + partial_value.astype(jnp.bfloat16).astype(jnp.float32)
    prompt_kv = (projected * inverse[:, None]).astype(jnp.bfloat16)
    target = block_owner[:, 0] * REQ_DEV + block_request
    labels = jnp.where(block_admit == 1, target, -1).astype(jnp.int32)
    token_labels = jnp.repeat(labels, BLK)
    prompt_rows = prompt_kv.astype(jnp.float32).reshape(PTOKENS, KVH, 2, HD)
    groups = QH // KVH
    factor = 1.0 / math.sqrt(HD)
    positions = jnp.arange(CACHE, dtype=jnp.int32)
    step_index = jnp.arange(STEPS, dtype=jnp.int32)
    causal = step_index[None, :] <= step_index[:, None]

    def one_request(items):
        ident, query, cache, length, draft = items
        qvec = query.astype(jnp.float32).reshape(STEPS, KVH, groups, HD)
        cached = cache.astype(jnp.float32).reshape(CACHE, KVH, 2, HD)
        drafted = draft.astype(jnp.float32).reshape(STEPS, KVH, 2, HD)
        keys = jnp.concatenate([cached[:, :, 0], prompt_rows[:, :, 0], drafted[:, :, 0]], axis=0)
        values = jnp.concatenate([cached[:, :, 1], prompt_rows[:, :, 1], drafted[:, :, 1]], axis=0)
        cache_ok = jnp.broadcast_to((positions < length)[None, :], (STEPS, CACHE))
        prompt_ok = jnp.broadcast_to((token_labels == ident)[None, :], (STEPS, PTOKENS))
        allowed = jnp.concatenate([cache_ok, prompt_ok, causal], axis=1)[:, None, None, :]
        scores = jnp.einsum('tkgd,nkd->tkgn', qvec, keys, precision=lax.Precision.HIGHEST) * factor
        masked = jnp.where(allowed, scores, -1e+30)
        highest = lax.optimization_barrier(jnp.max(masked, axis=-1))
        weights = jnp.where(allowed, jnp.exp(masked - highest[..., None]), 0.0)
        summed = jnp.einsum('tkgn,nkd->tkgd', weights, values, precision=lax.Precision.HIGHEST)
        result = summed / lax.optimization_barrier(jnp.sum(weights, axis=-1))[..., None]
        return result.reshape(STEPS, QH * HD).astype(jnp.bfloat16)
    idents = jnp.arange(REQUESTS, dtype=jnp.int32)
    return lax.map(one_request, (idents, queries, cache_kv, cache_len, draft_kv))
```

```python
import functools
import math

import jax
import jax.numpy as jnp
from jax import lax
from jax.experimental import pallas as pl
from jax.experimental.pallas import tpu as pltpu
from jax.sharding import PartitionSpec as P

D = 8192
KVH = 8
HD = 128
QH = 64
BLK = 16
CACHE = 2048
STEPS = 4
GROUPS = QH // KVH
ROWS = STEPS * GROUPS
SCALE = 1.0 / math.sqrt(HD)
NEG = -1e30


def absorb(state, scores, allowed, values, form):
    highest, total, summed = state
    masked = jnp.where(allowed, scores, NEG)
    new_top = jnp.maximum(highest, jnp.max(masked, axis=-1))
    weights = jnp.where(allowed, jnp.exp(masked - new_top[..., None]), 0.0)
    shrink = jnp.exp(highest - new_top)
    total = total * shrink + jnp.sum(weights, axis=-1)
    summed = summed * shrink[..., None] + jnp.einsum(
        form, weights, values.astype(jnp.float32), precision=lax.Precision.HIGHEST
    )
    return (new_top, total, summed)


def shared_keys(state, qvec, keys, values, allowed):
    scores = jnp.einsum("rskgd,nkd->rskgn", qvec, keys, preferred_element_type=jnp.float32) * SCALE
    return absorb(state, scores, allowed[:, None, None, None, :], values, "rskgn,nkd->rskgd")


def own_keys(state, qvec, keys, values, allowed):
    scores = jnp.einsum("rskgd,rnkd->rskgn", qvec, keys, preferred_element_type=jnp.float32) * SCALE
    return absorb(state, scores, allowed, values, "rskgn,rnkd->rskgd")


def general(
    prompt_states,
    norm_gain,
    kv_weight,
    block_owner,
    block_request,
    block_admit,
    cache_kv,
    cache_len,
    queries,
    draft_kv,
):
    wide = lax.axis_size("wide")
    states = prompt_states.astype(jnp.float32)
    squares = lax.psum(jnp.sum(states * states, axis=1), "mp")
    inverse = lax.rsqrt(squares / D + 1e-05)
    scaled = (states * norm_gain).astype(jnp.bfloat16)
    partial_kv = jnp.dot(
        scaled,
        lax.all_gather(kv_weight, "wide", axis=1, tiled=True),
        preferred_element_type=jnp.float32,
    )
    summed_kv = lax.psum_scatter(
        partial_kv.astype(jnp.bfloat16), "mp", scatter_dimension=1, tiled=True
    ).astype(jnp.float32)
    prompt_kv = (summed_kv * inverse[:, None]).astype(jnp.bfloat16)
    width = cache_kv.shape[2]
    heads_here = width // (2 * HD)
    req_dev = queries.shape[0]
    pblk = block_request.shape[0]
    blocks = prompt_kv.reshape(pblk, BLK, width)
    local_ids = jnp.arange(req_dev, dtype=jnp.int32)
    qvec = queries.reshape(req_dev, STEPS, heads_here, GROUPS, HD)
    state = (
        jnp.full((req_dev, STEPS, heads_here, GROUPS), NEG, jnp.float32),
        jnp.zeros((req_dev, STEPS, heads_here, GROUPS), jnp.float32),
        jnp.zeros((req_dev, STEPS, heads_here, GROUPS, HD), jnp.float32),
    )
    cached = cache_kv.reshape(req_dev, CACHE, heads_here, 2, HD)
    cache_ok = (jnp.arange(CACHE, dtype=jnp.int32)[None, :] < cache_len[:, None])[
        :, None, None, None, :
    ]
    state = own_keys(state, qvec, cached[:, :, :, 0], cached[:, :, :, 1], cache_ok)
    drafted = draft_kv.reshape(req_dev, STEPS, heads_here, 2, HD)
    step_index = jnp.arange(STEPS, dtype=jnp.int32)
    causal = (step_index[None, :] <= step_index[:, None])[None, :, None, None, :]
    state = own_keys(state, qvec, drafted[:, :, :, 0], drafted[:, :, :, 1], causal)
    owner = block_owner[:, 0]
    capacity = max(2, (2 * pblk + wide - 1) // wide)
    hits = (owner[:, None] == jnp.arange(wide, dtype=jnp.int32)[None, :]).astype(jnp.int32)
    slot = jnp.sum((jnp.cumsum(hits, axis=0) - hits) * hits, axis=1)
    outgoing = jnp.zeros((wide, capacity, BLK, width), jnp.bfloat16).at[owner, slot].set(blocks)
    tagged = jnp.where(block_admit == 1, block_request, -1)
    outgoing_labels = jnp.full((wide, capacity), -1, jnp.int32).at[owner, slot].set(tagged)
    incoming, arrived = (
        lax.all_to_all(outgoing, "wide", split_axis=0, concat_axis=0, tiled=True),
        lax.all_to_all(outgoing_labels, "wide", split_axis=0, concat_axis=0, tiled=True),
    )
    rows = incoming.reshape(-1, heads_here, 2, HD)
    token_labels = jnp.repeat(arrived.reshape(-1), BLK)
    allowed = token_labels[None, :] == local_ids[:, None]
    state = shared_keys(state, qvec, rows[:, :, 0], rows[:, :, 1], allowed)
    highest, total, summed = state
    result = summed / total[..., None]
    return result.reshape(req_dev, STEPS, heads_here * GROUPS * HD).astype(jnp.bfloat16)


NT = (((1,), (1,)), ((), ()))


def cached_kernel(len_ref, q_ref, cache_ref, draft_ref, o_ref, m_ref, l_ref):
    length = len_ref[pl.program_id(0)]
    rows_c = cache_ref.shape[1]
    rows_d = draft_ref.shape[1]
    for head in range(q_ref.shape[1]):
        at = head * 2 * HD
        q = q_ref[0, head]
        s = lax.dot_general(
            q, cache_ref[0, :, at : at + HD], NT, preferred_element_type=jnp.float32
        )
        ok = lax.broadcasted_iota(jnp.int32, (ROWS, rows_c), 1) < length
        s = jnp.where(ok, s * SCALE, NEG)
        d = lax.dot_general(
            q, draft_ref[0, :, at : at + HD], NT, preferred_element_type=jnp.float32
        )
        step = lax.broadcasted_iota(jnp.int32, (ROWS, rows_d), 0) // GROUPS
        seen = lax.broadcasted_iota(jnp.int32, (ROWS, rows_d), 1) <= step
        d = jnp.where(seen, d * SCALE, NEG)
        top = jnp.maximum(
            jnp.max(s, axis=1, keepdims=True), jnp.max(d, axis=1, keepdims=True)
        )
        ps = jnp.where(ok, jnp.exp(s - top), 0.0)
        pd = jnp.where(seen, jnp.exp(d - top), 0.0)
        total = jnp.sum(ps, axis=1, keepdims=True) + jnp.sum(pd, axis=1, keepdims=True)
        out = jnp.dot(
            ps.astype(jnp.bfloat16),
            cache_ref[0, :, at + HD : at + 2 * HD],
            preferred_element_type=jnp.float32,
        ) + jnp.dot(
            pd.astype(jnp.bfloat16),
            draft_ref[0, :, at + HD : at + 2 * HD],
            preferred_element_type=jnp.float32,
        )
        o_ref[0, head] = out
        m_ref[0, head] = jnp.broadcast_to(top, (ROWS, HD))
        l_ref[0, head] = jnp.broadcast_to(total, (ROWS, HD))


def cached_part(cache_len, q_heads, cache_kv, draft):
    req, heads = q_heads.shape[:2]
    shape = jax.ShapeDtypeStruct((req, heads, ROWS, HD), jnp.float32)
    spec = pl.BlockSpec((1, heads, ROWS, HD), lambda r, n: (r, 0, 0, 0))
    return pl.pallas_call(
        cached_kernel,
        out_shape=(shape,) * 3,
        grid_spec=pltpu.PrefetchScalarGridSpec(
            num_scalar_prefetch=1,
            grid=(req,),
            in_specs=[
                spec,
                pl.BlockSpec((1,) + cache_kv.shape[1:], lambda r, n: (r, 0, 0)),
                pl.BlockSpec((1,) + draft.shape[1:], lambda r, n: (r, 0, 0)),
            ],
            out_specs=[spec] * 3,
        ),
        cost_estimate=pl.CostEstimate(
            flops=8000000000, bytes_accessed=2 * cache_kv.size, transcendentals=300000
        ),
        name="cached",
    )(cache_len, q_heads, cache_kv, draft)


def score_kernel(q_ref, ka_ref, kb_ref, sq_ref, label_ref, p_ref, l_ref, lse_ref):
    tokens = ka_ref.shape[0] // 2
    rows = q_ref.shape[1]
    for part in range(2):
        span = slice(part * tokens, (part + 1) * tokens)
        keys = (
            ka_ref[span].astype(jnp.float32) + kb_ref[span].astype(jnp.float32)
        ).astype(jnp.bfloat16)
        inverse = lax.rsqrt(sq_ref[part] * (1.0 / D) + 1e-05)
        s = lax.dot_general(q_ref[part], keys, NT, preferred_element_type=jnp.float32)
        request = (lax.broadcasted_iota(jnp.int32, (rows, tokens), 0) // ROWS).astype(jnp.float32)
        ok = request == label_ref[part]
        s = jnp.where(ok, s * (inverse * SCALE), NEG)
        top = jnp.max(s, axis=1, keepdims=True)
        w = jnp.where(ok, jnp.exp(s - top), 0.0)
        total = jnp.sum(w, axis=1, keepdims=True)
        p_ref[part] = (w * inverse).astype(jnp.bfloat16)
        some = total > 0.0
        safe = jnp.where(some, total, 1.0)
        l_ref[part] = jnp.broadcast_to(1.0 / safe, (rows, HD))
        lse_ref[part] = jnp.broadcast_to(jnp.where(some, top + jnp.log(safe), NEG), (rows, HD))


def score_part(q_all, ka, kb, squares, labels):
    rows = q_all.shape[1]
    tokens = ka.shape[0] // 2
    stat = jax.ShapeDtypeStruct((2, rows, HD), jnp.float32)
    return pl.pallas_call(
        score_kernel,
        out_shape=(jax.ShapeDtypeStruct((2, rows, tokens), jnp.bfloat16), stat, stat),
        cost_estimate=pl.CostEstimate(
            flops=2000000000, bytes_accessed=2000000, transcendentals=300000
        ),
        name="scores",
    )(q_all, ka, kb, squares, labels)


def value_kernel(p_ref, va_ref, vb_ref, l_ref, lse_ref, out_ref):
    tokens = va_ref.shape[0] // 2
    for part in range(2):
        span = slice(part * tokens, (part + 1) * tokens)
        values = (
            va_ref[span].astype(jnp.float32) + vb_ref[span].astype(jnp.float32)
        ).astype(jnp.bfloat16)
        o = jnp.dot(p_ref[part], values, preferred_element_type=jnp.float32)
        out_ref[part, :, :HD] = o * l_ref[part]
        out_ref[part, :, HD:] = lse_ref[part]


def value_part(weights, va, vb, norm, lse):
    rows = weights.shape[1]
    return pl.pallas_call(
        value_kernel,
        out_shape=jax.ShapeDtypeStruct((2, rows, 2 * HD), jnp.float32),
        cost_estimate=pl.CostEstimate(
            flops=1000000000, bytes_accessed=2000000, transcendentals=0
        ),
        name="values",
    )(weights, va, vb, norm, lse)


def join_kernel(o_ref, m_ref, l_ref, got_ref, out_ref):
    heads, sources = got_ref.shape[:2]
    for req in range(o_ref.shape[0]):
        for head in range(heads):
            own_top = m_ref[req, head]
            top = own_top
            for i in range(sources):
                top = jnp.maximum(top, got_ref[head, i, req, :, HD:])
            share = jnp.exp(own_top - top)
            total = l_ref[req, head] * share
            summed = o_ref[req, head] * share
            for i in range(sources):
                share = jnp.exp(got_ref[head, i, req, :, HD:] - top)
                total = total + share
                summed = summed + got_ref[head, i, req, :, :HD] * share
            out_ref[req, head] = (summed / total).astype(jnp.bfloat16)


def join_part(o, m, l, got):
    return pl.pallas_call(
        join_kernel,
        out_shape=jax.ShapeDtypeStruct(o.shape, jnp.bfloat16),
        name="join",
    )(o, m, l, got)


def line_of_four(
    prompt_states,
    norm_gain,
    kv_weight,
    block_owner,
    block_request,
    block_admit,
    cache_kv,
    cache_len,
    queries,
    draft_kv,
):
    y = lax.axis_index("parts")
    z = lax.axis_index("wide")
    m = lax.axis_index("mp")
    swap = [(0, 1), (1, 0)]
    depth = kv_weight.shape[0]
    tokens = prompt_states.shape[0]
    req = queries.shape[0]
    wide = lax.axis_size("wide")

    own = [
        lax.dynamic_slice(kv_weight, (0, y * 2 * HD + i * HD), (depth, HD)) for i in range(2)
    ]
    up1 = [lax.ppermute(c, "wide", [(0, 1), (1, 2), (2, 3)]) for c in own]
    down1 = [lax.ppermute(c, "wide", [(1, 0), (2, 1), (3, 2)]) for c in own]
    other_states = lax.ppermute(prompt_states, "parts", swap)
    up2 = [lax.ppermute(c, "wide", [(1, 2), (2, 3)]) for c in up1]
    down2 = [lax.ppermute(c, "wide", [(1, 0), (2, 1)]) for c in down1]
    second = [jnp.where(z >= 2, u, d) for u, d in zip(up2, down2)]
    third = [lax.ppermute(c, "wide", [(1, 0), (2, 3)]) for c in second]
    ends = (z == 0) | (z == wide - 1)
    first = [jnp.where(z == 0, d, u) for u, d in zip(up1, down1)]
    last = [jnp.where(ends, t, d) for t, d in zip(third, down1)]

    mine = prompt_states.astype(jnp.float32)
    squares = lax.psum(jnp.sum(mine * mine, axis=1), "mp")
    label = jnp.where(block_admit == 1, block_owner[:, 0] * req + block_request, -1)
    facts = jnp.stack([squares, jnp.repeat(label, BLK).astype(jnp.float32)])
    facts = jnp.stack([facts, lax.ppermute(facts, "parts", swap)])
    sq_rows, label_rows = facts[:, 0:1], facts[:, 1:2]

    q_heads = queries.reshape(req, STEPS, 2, GROUPS, HD).transpose(0, 2, 1, 3, 4)
    q_heads = q_heads.reshape(req, 2, ROWS, HD)
    q_keep = lax.dynamic_index_in_dim(q_heads, y, 1, keepdims=False)
    q_send = lax.dynamic_index_in_dim(q_heads, 1 - y, 1, keepdims=False)
    q_pair = jnp.stack([q_keep, lax.ppermute(q_send, "parts", swap)])
    q_all = lax.all_gather(q_pair, "wide", axis=1, tiled=False)
    q_all = q_all.reshape(2, wide * req * ROWS, HD)

    draft = jnp.pad(draft_kv, ((0, 0), (0, 16 - STEPS), (0, 0)))
    o, top, total = cached_part(cache_len, q_heads, cache_kv, draft)

    scaled = (mine * norm_gain).astype(jnp.bfloat16)
    scaled_other = (other_states.astype(jnp.float32) * norm_gain).astype(jnp.bfloat16)
    scaled, scaled_other = lax.optimization_barrier((scaled, scaled_other))
    both = jnp.concatenate([scaled, scaled_other], axis=0)

    where_is = jnp.array([[0, 1, 2, 3], [1, 0, 3, 2], [2, 1, 0, 3], [3, 2, 1, 0]], jnp.int32)[z]
    core, chip = m % 2, m // 2

    def reduced(index):
        slots = jnp.stack(
            [
                jnp.dot(both, c[index], preferred_element_type=jnp.float32).astype(jnp.bfloat16)
                for c in (own, first, second, last)
            ]
        )

        def target(x, c):
            return lax.dynamic_index_in_dim(slots, where_is[2 * x + c], 0, keepdims=False)

        sent = jnp.stack([target(0, 1 - core), target(1, 1 - core)])
        got = lax.ppermute(sent, "mp", [(0, 1), (1, 0), (2, 3), (3, 2)])
        kept = jnp.stack([target(0, core), target(1, core)])
        pair = (kept.astype(jnp.float32) + got.astype(jnp.float32)).astype(jnp.bfloat16)
        a = lax.dynamic_index_in_dim(pair, chip, 0, keepdims=False)
        b = lax.dynamic_index_in_dim(pair, 1 - chip, 0, keepdims=False)
        return a, lax.ppermute(b, "mp", [(0, 2), (2, 0), (1, 3), (3, 1)])

    ka, kb = reduced(0)
    weights, norm, lse = score_part(q_all, ka, kb, sq_rows, label_rows)
    va, vb = reduced(1)
    part = value_part(weights, va, vb, norm, lse)

    part = part.reshape(2, wide, req, ROWS, 2 * HD)
    part = jnp.where(y == 0, part, part[::-1])
    got = lax.all_to_all(
        part.reshape((2 * wide,) + part.shape[2:]), ("parts", "wide"), 0, 0, tiled=True
    )
    got = got.reshape((2, wide) + part.shape[2:])
    result = join_part(o, top, total, got)
    result = result.reshape(req, 2, STEPS, GROUPS, HD).transpose(0, 2, 1, 3, 4)
    return result.reshape(req, STEPS, 2 * GROUPS * HD)


def solution(mesh):
    placed = (
        P(("parts", "wide"), "mp"),
        P("mp"),
        P("mp", "wide"),
        P(("parts", "wide"), None),
        P(("parts", "wide")),
        P(("parts", "wide")),
        P(("parts", "wide"), None, "mp"),
        P(("parts", "wide")),
        P(("parts", "wide"), None, "mp"),
        P(("parts", "wide"), None, "mp"),
    )
    sizes = dict(mesh.shape)
    short = sizes["parts"] == 2 and sizes["wide"] == 4 and sizes["mp"] == 4
    return jax.shard_map(
        line_of_four if short else general,
        mesh=mesh,
        in_specs=placed,
        out_specs=P(("parts", "wide"), None, "mp"),
        check_vma=False,
    )
```
